128 devices in a mesh: node: 16 (over z, x), expert: 8 (over y, core).
Axes of the slice: x: 4, y: 4, z: 4, core: 2. Of those that a mesh axis runs over, the one named last changes fastest.
Arguments:
- tokens: bfloat16 [65536, 1024], P(('node', 'expert')), may hold values from -6 to 6
- queries: bfloat16 [65536, 1024], P(('node', 'expert')), may hold values from -6 to 6
- keys: bfloat16 [65536, 1024], P(('node', 'expert')), may hold values from -6 to 6
- values: bfloat16 [65536, 1024], P(('node', 'expert')), may hold values from -12 to 12
- neighbours: int32 [512, 8], P(('node', 'expert')), may hold values from 0 to 511, as said below
- live_bits: int32 [512, 8], P(('node', 'expert')), may hold values from 0 to 1, as said below
- out_proj: bfloat16 [1024, 1024], replicated, may hold values from -0.1875 to 0.1875
- norm_gain: float32 [1024], replicated, may hold values from 0.5 to 1.5
- router: bfloat16 [1024, 128], replicated, may hold values from -0.1875 to 0.1875
- expert: int32 [65536], P(('node', 'expert')), may hold values from 0 to 127, as said below
- slot: int32 [65536], P(('node', 'expert')), may hold values from 0 to 7, as said below
- w_up: bfloat16 [128, 1024, 4096], P(('node', 'expert')), may hold values from -0.1875 to 0.1875
- w_down: bfloat16 [128, 4096, 1024], P(('node', 'expert')), may hold values from -0.09375 to 0.09375
Outputs:
- layer_out: bfloat16 [65536, 1024], P(('node', 'expert'))
The draws below stay inside these ranges and needn't reach their ends.
Inputs may be any that keep to these rules, and one draw needn't show every extreme that they name: Tile g is held by device g // 4 in node-major order. neighbours[g, 0] is g itself; every listed tile is held by g's device or by the device one step before or after it along node with the same expert index (wrapping around); entry 1 is always one step before and entry 2 one step after. `live_bits`: entry 0 of every row is 1. Within the 512 tokens of one device, no two tokens share both expert and slot; some expert takes all 8 slots of every device. See expert: pairs (expert, slot) are distinct within one device's tokens.
All inputs are finite; a program needn't handle non-finite values.
Results may differ from the reference program's by a relative error of at most 0.0049.
Values may be sent and summed in bfloat16 or wider, within the bound.
A program may use at most 192 MiB of HBM per device.

```python
import jax
import jax.numpy as jnp
from jax import lax

D = 1024
HEADS = 16
HEAD_DIM = 64
FF = 4096
TILE = 128
NB = 8
TOK_DEV = 512
EXPERTS = 128
CAP = 8
TOKENS = 65536
TILES = 512
N_NODE = 16
N_EXPERT = 8
DEVICES = 128


def query_key_pair(key):
    base_query = jnp.clip(jax.random.normal(jax.random.fold_in(key, 31), (TOKENS, D), jnp.float32) * 1.3, -6.0, 6.0)
    base_key = jnp.clip(jax.random.normal(jax.random.fold_in(key, 32), (TOKENS, D), jnp.float32) * 1.3, -6.0, 6.0)
    return (base_query, base_key)


def draw_queries(key, part):
    return query_key_pair(key)[0].astype(jnp.bfloat16)


def draw_keys(key, part):
    return query_key_pair(key)[1].astype(jnp.bfloat16)


def draw_neighbours(key, part):
    tile_count = TOKENS // TILE
    tiles_dev = TOK_DEV // TILE
    tile_ids = jnp.arange(tile_count, dtype=jnp.int32)
    device_of = tile_ids // tiles_dev
    node_of = device_of // N_EXPERT
    column_of = device_of % N_EXPERT
    steps = jax.random.randint(key, (tile_count, NB), -1, 2, jnp.int32)
    steps = steps.at[:, 0].set(0).at[:, 1].set(-1).at[:, 2].set(1)
    picks = jax.random.randint(jax.random.fold_in(key, 1), (tile_count, NB), 0, tiles_dev, jnp.int32)
    other_device = (node_of[:, None] + steps + N_NODE) % N_NODE * N_EXPERT + column_of[:, None]
    listed = other_device * tiles_dev + picks
    listed = listed.at[:, 0].set(tile_ids)
    return listed.astype(jnp.int32)


def draw_live_bits(key, part):
    tile_count = TOKENS // TILE
    drawn = jax.random.randint(jax.random.fold_in(key, 5), (tile_count, NB), 0, 4, jnp.int32)
    bits = jnp.where(drawn > 0, 1, 0).astype(jnp.int32)
    return bits.at[:, 0].set(1)


def route_cells(key):
    block_count = TOKENS // TOK_DEV
    cell_count = EXPERTS * CAP
    noise = jax.random.randint(jax.random.fold_in(key, 21), (block_count, cell_count), 0, 2 ** 18, jnp.int32)
    heat = jax.random.randint(jax.random.fold_in(key, 22), (EXPERTS,), 0, 2 ** 18, jnp.int32)
    hottest = jax.random.randint(jax.random.fold_in(key, 23), (), 0, EXPERTS, jnp.int32)
    owner_of = jnp.arange(cell_count, dtype=jnp.int32) // CAP
    scores = noise + heat[owner_of][None, :] + jnp.where(owner_of == hottest, 2 ** 19, 0)[None, :]
    ranked = jnp.argsort(-scores, axis=1, stable=True)[:, :TOK_DEV]
    return ranked.reshape(TOKENS).astype(jnp.int32)


def draw_expert(key, part):
    return (route_cells(key) // CAP).astype(jnp.int32)


def draw_slot(key, part):
    return (route_cells(key) % CAP).astype(jnp.int32)


def block_scale(key, extent, split, least, top_value):
    def one(position, parts):
        draws = jax.random.uniform(jax.random.fold_in(jax.random.fold_in(key, 6), position), (parts,), jnp.float32, least / len(split), top_value / len(split))
        return jnp.repeat(jnp.exp(draws), extent[position] // parts).reshape((-1,) + (1,) * (len(extent) - position - 1))

    loudness = one(*split[0])
    for cut in split[1:]:
        loudness = loudness * one(*cut)
    return loudness


def scatter_about(rng, extent, deviation, bound, pieces=(), held_as=jnp.bfloat16):
    values = jax.random.normal(rng, extent, jnp.float32) * deviation
    if len(pieces) > 0:
        values = block_scale(rng, extent, pieces, -0.22, 0.18) * values
    return jnp.clip(values, min=-bound, max=bound).astype(held_as)


def setup_inputs(seed: int = 0) -> dict:
    seeds = jax.random.split(jax.random.key(seed), 14)
    tokens = scatter_about(seeds[0], (TOKENS, D), 1.0, 6.0, ((0, 128),))
    queries = draw_queries(jax.random.fold_in(seeds[13], 71), 0)
    keys = draw_keys(jax.random.fold_in(seeds[13], 71), 0)
    values = scatter_about(seeds[3], (TOKENS, D), 2.0, 12.0, ((0, 128),))
    neighbours = draw_neighbours(jax.random.fold_in(seeds[13], 71), 0)
    live_bits = draw_live_bits(jax.random.fold_in(seeds[13], 71), 0)
    out_proj = scatter_about(seeds[6], (D, D), D ** -0.5, 0.1875)
    norm_gain = jnp.clip(1.0 + 0.1 * jax.random.normal(seeds[7], (D,), jnp.float32), 0.5, 1.5)
    router = scatter_about(seeds[8], (D, EXPERTS), D ** -0.5, 0.1875)
    expert = draw_expert(jax.random.fold_in(seeds[13], 71), 0)
    slot = draw_slot(jax.random.fold_in(seeds[13], 71), 0)
    w_up = scatter_about(seeds[11], (EXPERTS, D, FF), D ** -0.5, 0.1875, ((0, 128),))
    w_down = scatter_about(seeds[12], (EXPERTS, FF, D), FF ** -0.5, 0.09375, ((0, 128),))
    return dict(tokens=tokens, queries=queries, keys=keys, values=values, neighbours=neighbours, live_bits=live_bits, out_proj=out_proj, norm_gain=norm_gain, router=router, expert=expert, slot=slot, w_up=w_up, w_down=w_down)


score_scale = 0.125

def attend_tile(packed, key_tiles, value_tiles):
    query_tile, listed, bits = packed
    near_keys = key_tiles[listed].reshape(NB * TILE, HEADS, HEAD_DIM).astype(jnp.float32)
    near_values = value_tiles[listed].reshape(NB * TILE, HEADS, HEAD_DIM).astype(jnp.float32)
    query_heads = query_tile.reshape(TILE, HEADS, HEAD_DIM).astype(jnp.float32)
    scores = jnp.einsum('qhd,khd->hqk', query_heads, near_keys) * score_scale
    visible = jnp.repeat(bits, TILE) > 0
    masked = jnp.where(visible[None, None, :], scores, -jnp.inf)
    peak = lax.optimization_barrier(jnp.max(masked, axis=-1, keepdims=True))
    weights = jnp.exp(masked - peak)
    weights = (weights / lax.optimization_barrier(jnp.sum(weights, axis=-1, keepdims=True))).astype(jnp.bfloat16)
    mixed = jnp.einsum('hqk,khd->qhd', weights.astype(jnp.float32), near_values)
    return mixed.reshape(TILE, D).astype(jnp.bfloat16)

def reference(tokens, queries, keys, values, neighbours, live_bits, out_proj, norm_gain, router, expert, slot, w_up, w_down):
    key_tiles = keys.reshape(TILES, TILE, D)
    value_tiles = values.reshape(TILES, TILE, D)
    query_tiles = queries.reshape(TILES, TILE, D)
    attn = lax.map(lambda packed: attend_tile(packed, key_tiles, value_tiles), (query_tiles, neighbours, live_bits))
    attn = attn.reshape(TOKENS, D)
    hidden = tokens.astype(jnp.float32) + jnp.dot(attn, out_proj, preferred_element_type=jnp.float32)
    spread = lax.optimization_barrier(jnp.mean(hidden * hidden, axis=-1, keepdims=True))
    normed = (hidden * lax.rsqrt(spread + 1e-06) * norm_gain.astype(jnp.float32)[None, :]).astype(jnp.bfloat16)
    logits = jnp.dot(normed, router, preferred_element_type=jnp.float32)
    columns = jnp.arange(EXPERTS, dtype=jnp.int32)
    chosen = lax.optimization_barrier(jnp.sum(jnp.where(columns[None, :] == expert[:, None], logits, 0.0), axis=-1))
    gate = jax.nn.sigmoid(chosen)
    positions = jnp.arange(TOKENS, dtype=jnp.int32)
    target = expert * (DEVICES * CAP) + positions // TOK_DEV * CAP + slot
    table = jnp.full((EXPERTS * DEVICES * CAP,), TOKENS, jnp.int32).at[target].set(positions)
    padded = jnp.concatenate([normed, jnp.zeros((1, D), jnp.bfloat16)], axis=0)

    def run_expert(packed):
        index_rows, up_matrix, down_matrix = packed
        token_rows = padded[index_rows]
        lifted = jnp.dot(token_rows, up_matrix, preferred_element_type=jnp.float32)
        lifted = jax.nn.gelu(lifted, approximate=True).astype(jnp.bfloat16)
        return jnp.dot(lifted, down_matrix, preferred_element_type=jnp.float32).astype(jnp.bfloat16)
    results = lax.map(run_expert, (table.reshape(EXPERTS, DEVICES * CAP), w_up, w_down))
    expert_out = results.reshape(EXPERTS * DEVICES * CAP, D)[target]
    layer_out = hidden + gate[:, None] * expert_out.astype(jnp.float32)
    return layer_out.astype(jnp.bfloat16)
```

```python
import functools

import jax
import jax.numpy as jnp
from jax import lax
from jax.experimental import pallas as pl
from jax.experimental.pallas import tpu as pltpu
from jax.sharding import PartitionSpec as P

MESH = pl.DeviceIdType.MESH
D = 1024
HEADS = 16
HEAD_DIM = 64
FF = 4096
TILE = 128
NB = 8
TOK = 512
TILES = TOK // TILE
CAP = 8
DEVICES = 128
N_NODE = 16
N_EXPERT = 8
LANES = 128
CHUNKS = D // LANES
PARTS = 4
PART_DEVICES = DEVICES // PARTS
PART_ROWS = PART_DEVICES * CAP
FF_BLOCK = 512
OUT_BLOCK = 256
SCALE = 0.125 * 1.4426950408889634
GELU_A = 0.7978845608028654
GELU_B = 0.044715 * GELU_A


def gelu(v):
    return (0.5 * v) * (1.0 + jnp.tanh(v * (GELU_A + GELU_B * (v * v))))


def offset_of(part, i):
    core = i % 2
    z = (i // 2) % 4
    x = i // 8
    y = (part + z + x) % 4
    return z, x, y, core


def kernel(
    nbr_ref, live_ref, tok_hbm, q_hbm, k_hbm, v_hbm, wo_hbm, gain_ref, router_ref, expert_ref, slot_ref, up_hbm, down_hbm,
    out_hbm,
    kv, q_v, tok_v, wo_v, attn_v, near_k, near_v, hidden_v, normed_v, gate_v, col_v,
    send_v, recv_v, res_v, ret_v, up_v, down_v, lifted_v, acc_v, out_v,
    load_sem, kv_sem, q_sem, w_sem, halo_send, halo_recv, disp_send, disp_recv, ret_send, ret_recv, self_sem, out_sem,
):
    node = lax.axis_index("node")
    column = lax.axis_index("expert")
    z, x, y, core = node // 4, node % 4, column // 2, column % 2

    def device(dz, dx, dy, dc):
        return ((z + dz) % 4 * 4 + (x + dx) % 4, (y + dy) % 4 * 2 + (core + dc) % 2)

    barrier = pltpu.get_barrier_semaphore()

    def greet(i, carry):
        pl.semaphore_signal(
            barrier, inc=1, device_id=((node + i // N_EXPERT) % N_NODE, (column + i % N_EXPERT) % N_EXPERT), device_id_type=MESH
        )
        return carry

    lax.fori_loop(1, DEVICES, greet, 0)

    def kv_load(c, which):
        source = k_hbm if which == 0 else v_hbm
        return pltpu.make_async_copy(
            source.at[:, pl.ds(pl.multiple_of(c * LANES, LANES), LANES)], kv.at[0, c, which], kv_sem.at[c, which]
        )

    def start_kv(c, carry):
        kv_load(c, 0).start()
        kv_load(c, 1).start()
        return carry

    lax.fori_loop(0, CHUNKS, start_kv, 0)

    def q_load(c):
        return pltpu.make_async_copy(
            q_hbm.at[:, pl.ds(pl.multiple_of(c * LANES, LANES), LANES)], q_v.at[c], q_sem.at[c]
        )

    def start_q(c, carry):
        q_load(c).start()
        return carry

    lax.fori_loop(0, CHUNKS, start_q, 0)
    tok_load = pltpu.make_async_copy(tok_hbm, tok_v, load_sem.at[0])
    wo_load = pltpu.make_async_copy(wo_hbm, wo_v, load_sem.at[1])
    up_load = pltpu.make_async_copy(up_hbm.at[0], up_v, w_sem.at[0])
    down_load = pltpu.make_async_copy(down_hbm.at[0], down_v, w_sem.at[1])

    pl.semaphore_wait(barrier, DEVICES - 1)

    after = ((node + 1) % N_NODE, column)
    before = ((node + N_NODE - 1) % N_NODE, column)

    def halo(c, side):
        return pltpu.make_async_remote_copy(
            src_ref=kv.at[0, c], dst_ref=kv.at[1 + side, c], send_sem=halo_send.at[side, c], recv_sem=halo_recv.at[side, c],
            device_id=after if side == 0 else before, device_id_type=MESH,
        )

    def start_halo(c, carry):
        kv_load(c, 0).wait()
        kv_load(c, 1).wait()
        halo(c, 0).start()
        halo(c, 1).start()
        return carry

    lax.fori_loop(0, CHUNKS, start_halo, 0)
    tok_load.start()
    wo_load.start()
    up_load.start()
    down_load.start()

    lane = lax.broadcasted_iota(jnp.int32, (TILE, LANES), 1)
    left = lane < HEAD_DIM
    left_mask = jnp.where(left, 1.0, 0.0).astype(jnp.bfloat16)
    right_mask = jnp.where(left, 0.0, 1.0).astype(jnp.bfloat16)

    def attend(c, carry):
        halo(c, 0).wait_recv()
        halo(c, 1).wait_recv()
        q_load(c).wait()
        for b in range(3):
            near_k[pl.ds(b * TILES, TILES)] = kv[b, c, 0].reshape(TILES, TILE, LANES)
            near_v[pl.ds(b * TILES, TILES)] = kv[b, c, 1].reshape(TILES, TILE, LANES)
        for t in range(TILES):
            own = nbr_ref[t, 0] % TILES
            key_tiles = []
            value_tiles = []
            for j in range(NB):
                listed = nbr_ref[t, j]
                step = (listed // (TILES * N_EXPERT) - node + N_NODE) % N_NODE
                block = jnp.where(step == 0, 0, jnp.where(step == 1, 2, 1))
                bit = live_ref[t, j]
                position = jnp.where(bit > 0, block * TILES + listed % TILES, own)
                key_tiles.append(near_k[position])
                shown = jnp.full((TILE, LANES), jnp.where(bit > 0, 1.0, 0.0), jnp.float32).astype(jnp.bfloat16)
                value_tiles.append(jnp.concatenate([near_v[position] * shown, shown], axis=1))
            near_keys = jnp.concatenate(key_tiles, axis=0)
            near_values = jnp.concatenate(value_tiles, axis=0)
            rows = pl.ds(t * TILE, TILE)
            query = q_v[c, rows, :]
            both = jnp.concatenate([query * left_mask, query * right_mask], axis=0)
            scores = lax.dot_general(both, near_keys, (((1,), (1,)), ((), ())), preferred_element_type=jnp.float32)
            peak = jnp.max(scores, axis=1, keepdims=True)
            weights = jnp.exp2((scores - peak) * SCALE).astype(jnp.bfloat16)
            mixed = jnp.dot(weights, near_values, preferred_element_type=jnp.float32)
            ratio = mixed[:, :LANES] / mixed[:, LANES:]
            attn_v[rows, pl.ds(pl.multiple_of(c * LANES, LANES), LANES)] = jnp.where(
                left, ratio[:TILE], ratio[TILE:]
            ).astype(jnp.bfloat16)
        return carry

    lax.fori_loop(0, CHUNKS, attend, 0)

    tok_load.wait()
    wo_load.wait()

    def project(t, carry):
        rows = pl.ds(pl.multiple_of(t * TILE, TILE), TILE)
        hidden = tok_v[rows, :].astype(jnp.float32) + jnp.dot(attn_v[rows, :], wo_v[...], preferred_element_type=jnp.float32)
        hidden_v[rows, :] = hidden
        spread = jnp.mean(hidden * hidden, axis=1, keepdims=True)
        normed = (hidden * lax.rsqrt(spread + 1e-06) * gain_ref[...]).astype(jnp.bfloat16)
        normed_v[rows, :] = normed
        logits = jnp.dot(normed, router_ref[...], preferred_element_type=jnp.float32)
        chosen_row = jnp.broadcast_to(expert_ref[pl.ds(t, 1), :].astype(jnp.float32), (TILE, LANES))
        chosen = jnp.where(lane.astype(jnp.float32) == chosen_row.T, logits, 0.0)
        gate_v[rows, :] = jnp.broadcast_to(jax.nn.sigmoid(jnp.sum(chosen, axis=1, keepdims=True)), (TILE, LANES))
        return carry

    lax.fori_loop(0, TILES, project, 0)

    owner = expert_ref[...]
    dc = (owner % 2 - core + 2) % 2
    dy = (owner // 2 % 4 - y + 4) % 4
    dx = (owner // 8 % 4 - x + 4) % 4
    dz = (owner // 32 - z + 4) % 4
    part_of = (dy + 8 - dz - dx) % 4
    cell = ((part_of * PART_DEVICES + dx * 8 + dz * 2 + dc) * CAP + slot_ref[...]).astype(jnp.float32)
    for t in range(TILES):
        col_v[pl.ds(t * TILE, TILE), :] = jnp.broadcast_to(cell[t : t + 1, :], (TILE, LANES)).T
    cell_row = jnp.concatenate([cell[t : t + 1, :] for t in range(TILES)], axis=1)

    def dispatch(part, i):
        oz, ox, oy, oc = offset_of(part, i)
        at = part * PART_DEVICES + i
        return pltpu.make_async_remote_copy(
            src_ref=send_v.at[at], dst_ref=recv_v.at[at], send_sem=disp_send.at[part], recv_sem=disp_recv.at[part],
            device_id=device(oz, ox, oy, oc), device_id_type=MESH,
        )

    own_copy = pltpu.make_async_copy(send_v.at[0], recv_v.at[0], self_sem.at[0])
    for part in range(PARTS):
        wanted = lax.broadcasted_iota(jnp.int32, (PART_ROWS, TOK), 0).astype(jnp.float32) + part * PART_ROWS
        one_hot = jnp.where(wanted == cell_row, 1.0, 0.0).astype(jnp.bfloat16)
        rows = jnp.dot(one_hot, normed_v[...], preferred_element_type=jnp.float32).astype(jnp.bfloat16)
        send_v[pl.ds(part * PART_DEVICES, PART_DEVICES)] = rows.reshape(PART_DEVICES, CAP, D)

        def start_dispatch(i, carry, part=part):
            dispatch(part, i).start()
            return carry

        lax.fori_loop(1 if part == 0 else 0, PART_DEVICES, start_dispatch, 0)
        if part == 0:
            own_copy.start()

    up_load.wait()
    down_load.wait()

    def give_back(part, i):
        oz, ox, oy, oc = offset_of(part, i)
        at = part * PART_DEVICES + i
        return pltpu.make_async_remote_copy(
            src_ref=res_v.at[at], dst_ref=ret_v.at[at], send_sem=ret_send.at[part], recv_sem=ret_recv.at[part],
            device_id=device(4 - oz, 4 - ox, 4 - oy, 2 - oc), device_id_type=MESH,
        )

    own_back = pltpu.make_async_copy(res_v.at[0], ret_v.at[0], self_sem.at[1])

    def part_slice(part):
        first = part * PART_DEVICES + (1 if part == 0 else 0)
        return pl.ds(first, PART_DEVICES - (1 if part == 0 else 0))

    for part in range(PARTS):
        if part == 0:
            own_copy.wait()
        pltpu.make_async_copy(recv_v.at[part_slice(part)], recv_v.at[part_slice(part)], disp_recv.at[part]).wait()
        here = pl.ds(part * PART_DEVICES, PART_DEVICES)

        def lift(f, carry):
            columns = pl.ds(pl.multiple_of(f * FF_BLOCK, FF_BLOCK), FF_BLOCK)
            rows = recv_v[here].reshape(PART_ROWS, D)
            lifted_v[:, columns] = gelu(
                jnp.dot(rows, up_v[:, columns], preferred_element_type=jnp.float32)
            ).astype(jnp.bfloat16)
            return carry

        lax.fori_loop(0, FF // FF_BLOCK, lift, 0)

        def lower(n, carry):
            columns = pl.ds(pl.multiple_of(n * OUT_BLOCK, OUT_BLOCK), OUT_BLOCK)
            lowered = jnp.dot(lifted_v[...], down_v[:, columns], preferred_element_type=jnp.float32)
            res_v[here, :, columns] = lowered.astype(jnp.bfloat16).reshape(PART_DEVICES, CAP, OUT_BLOCK)
            return carry

        lax.fori_loop(0, D // OUT_BLOCK, lower, 0)

        def start_back(i, carry, part=part):
            give_back(part, i).start()
            return carry

        lax.fori_loop(1 if part == 0 else 0, PART_DEVICES, start_back, 0)
        if part == 0:
            own_back.start()

    for part in range(PARTS):
        if part == 0:
            own_back.wait()
        pltpu.make_async_copy(ret_v.at[part_slice(part)], ret_v.at[part_slice(part)], ret_recv.at[part]).wait()
        here = pl.ds(part * PART_DEVICES, PART_DEVICES)
        for t in range(TILES):
            rows = pl.ds(t * TILE, TILE)
            place = col_v[rows, :]
            one_hot = jnp.concatenate(
                [
                    jnp.where(place == lane.astype(jnp.float32) + (part * PART_ROWS + s * LANES), 1.0, 0.0).astype(jnp.bfloat16)
                    for s in range(PART_ROWS // LANES)
                ],
                axis=1,
            )
            taken = jnp.dot(one_hot, ret_v[here].reshape(PART_ROWS, D), preferred_element_type=jnp.float32)
            if part == 0:
                acc_v[rows, :] = taken
            elif part < PARTS - 1:
                acc_v[rows, :] += taken
            else:
                gate = gate_v[rows, :1]
                out_v[rows, :] = (hidden_v[rows, :] + gate * (acc_v[rows, :] + taken)).astype(jnp.bfloat16)

    store = pltpu.make_async_copy(out_v, out_hbm, out_sem)
    store.start()

    def end_halo(c, carry):
        halo(c, 0).wait_send()
        halo(c, 1).wait_send()
        return carry

    lax.fori_loop(0, CHUNKS, end_halo, 0)
    for part in range(PARTS):
        pltpu.make_async_copy(send_v.at[part_slice(part)], send_v.at[part_slice(part)], disp_send.at[part]).wait()
        pltpu.make_async_copy(res_v.at[part_slice(part)], res_v.at[part_slice(part)], ret_send.at[part]).wait()
    store.wait()


def shards(tokens, queries, keys, values, neighbours, live_bits, out_proj, norm_gain, router, expert, slot, w_up, w_down):
    any_spec = pl.BlockSpec(memory_space=pltpu.HBM)
    smem = pl.BlockSpec(memory_space=pltpu.SMEM)
    vmem = pl.BlockSpec(memory_space=pltpu.VMEM)
    bf16, f32 = jnp.bfloat16, jnp.float32
    dma = pltpu.SemaphoreType.DMA
    return pl.pallas_call(
        kernel,
        name="layer",
        out_shape=jax.ShapeDtypeStruct((TOK, D), bf16),
        in_specs=[smem, smem] + [any_spec] * 5 + [vmem] * 4 + [any_spec] * 2,
        out_specs=any_spec,
        scratch_shapes=[
            pltpu.VMEM((3, CHUNKS, 2, TOK, LANES), bf16),
            pltpu.VMEM((CHUNKS, TOK, LANES), bf16),
            pltpu.VMEM((TOK, D), bf16),
            pltpu.VMEM((D, D), bf16),
            pltpu.VMEM((TOK, D), bf16),
            pltpu.VMEM((3 * TILES, TILE, LANES), bf16),
            pltpu.VMEM((3 * TILES, TILE, LANES), bf16),
            pltpu.VMEM((TOK, D), f32),
            pltpu.VMEM((TOK, D), bf16),
            pltpu.VMEM((TOK, LANES), f32),
            pltpu.VMEM((TOK, LANES), f32),
            pltpu.VMEM((DEVICES, CAP, D), bf16),
            pltpu.VMEM((DEVICES, CAP, D), bf16),
            pltpu.VMEM((DEVICES, CAP, D), bf16),
            pltpu.VMEM((DEVICES, CAP, D), bf16),
            pltpu.VMEM((D, FF), bf16),
            pltpu.VMEM((FF, D), bf16),
            pltpu.VMEM((PART_ROWS, FF), bf16),
            pltpu.VMEM((TOK, D), f32),
            pltpu.VMEM((TOK, D), bf16),
            dma((2,)),
            dma((CHUNKS, 2)),
            dma((CHUNKS,)),
            dma((2,)),
            dma((2, CHUNKS)),
            dma((2, CHUNKS)),
            dma((PARTS,)),
            dma((PARTS,)),
            dma((PARTS,)),
            dma((PARTS,)),
            dma((2,)),
            dma,
        ],
        compiler_params=pltpu.CompilerParams(collective_id=0, has_side_effects=True, vmem_limit_bytes=64_000_000),
    )(
        neighbours, live_bits, tokens, queries, keys, values, out_proj, norm_gain.reshape(1, D), router,
        expert.reshape(TILES, TILE), slot.reshape(TILES, TILE), w_up, w_down,
    )


def solution(mesh):
    rows = P(("node", "expert"), None)
    flat = P(("node", "expert"))
    deep = P(("node", "expert"), None, None)
    in_specs = (rows, rows, rows, rows, rows, rows, P(), P(), P(), flat, flat, deep, deep)
    return jax.shard_map(shards, mesh=mesh, in_specs=in_specs, out_specs=rows, check_vma=False)
```

```python
import functools

import jax
import jax.numpy as jnp
from jax import lax
from jax.experimental import pallas as pl
from jax.experimental.pallas import tpu as pltpu
from jax.sharding import PartitionSpec as P

MESH = pl.DeviceIdType.MESH
D = 1024
HEADS = 16
HEAD_DIM = 64
FF = 4096
TILE = 128
NB = 8
TOK = 512
TILES = TOK // TILE
CAP = 8
DEVICES = 128
N_NODE = 16
N_EXPERT = 8
LANES = 128
CHUNKS = D // LANES
PARTS = 4
PART_DEVICES = DEVICES // PARTS
PART_ROWS = PART_DEVICES * CAP
FF_BLOCK = 1024
OUT_BLOCK = 512
VMEM_LIMIT = 58_000_000
SCALE = 0.125 * 1.4426950408889634
GELU_A = 0.7978845608028654
GELU_B = 0.044715 * GELU_A


def gelu(v):
    return (0.5 * v) * (1.0 + jnp.tanh(v * (GELU_A + GELU_B * (v * v))))


def offset_of(part, i):
    core = i % 2
    z = (i // 2) % 4
    x = i // 8
    return z, x, z + x, core


def kernel(
    nbr_hbm, live_hbm, tok_hbm, q_hbm, k_hbm, v_hbm, wo_hbm, gain_hbm, router_hbm, expert_hbm, slot_hbm, up_hbm, down_hbm,
    out_ref,
    nbr_ref, live_ref, gain_v, router_v, expert_v, slot_v,
    kv, q_v, tok_v, wo_v, attn_v, near_k, near_v, weights_v, hidden_v, normed_v, gate_v, col_v,
    send_v, recv_v, res_v, ret_v, up_v, down_v, lifted_v, acc_v,
    load_sem, kv_sem, q_sem, halo_send, halo_recv, disp_send, disp_recv, ret_send, ret_recv, row_sem,
):
    node = lax.axis_index("node")
    column = lax.axis_index("expert")
    z, x, y, core = node // 4, node % 4, column // 2, column % 2

    def kv_load(c, which):
        source = k_hbm if which == 0 else v_hbm
        return pltpu.make_async_copy(
            source.at[:, pl.ds(pl.multiple_of(c * LANES, LANES), LANES)], kv.at[0, c, which], kv_sem.at[c, which]
        )

    def start_kv(c, carry):
        kv_load(c, 0).start()
        kv_load(c, 1).start()
        return carry

    lax.fori_loop(0, CHUNKS, start_kv, 0)

    barrier = pltpu.get_barrier_semaphore()
    for step in (1, N_NODE - 1) + tuple(range(2, N_NODE - 1)):
        pl.semaphore_signal(barrier, inc=1, device_id=((node + step) % N_NODE, column), device_id_type=MESH)
    for step in range(1, N_EXPERT):
        pl.semaphore_signal(barrier, inc=1, device_id=(node, (column + step) % N_EXPERT), device_id_type=MESH)

    def q_load(c):
        return pltpu.make_async_copy(
            q_hbm.at[:, pl.ds(pl.multiple_of(c * LANES, LANES), LANES)], q_v.at[c], q_sem.at[c]
        )

    def start_q(c, carry):
        q_load(c).start()
        return carry

    small_loads = [
        pltpu.make_async_copy(source, target, load_sem.at[4 + i])
        for i, (source, target) in enumerate(
            (
                (nbr_hbm, nbr_ref), (live_hbm, live_ref), (gain_hbm, gain_v), (router_hbm, router_v),
                (expert_hbm, expert_v), (slot_hbm, slot_v),
            )
        )
    ]
    tok_load = pltpu.make_async_copy(tok_hbm, tok_v, load_sem.at[0])
    wo_load = pltpu.make_async_copy(wo_hbm, wo_v, load_sem.at[1])
    up_load = pltpu.make_async_copy(up_hbm.at[0], up_v, load_sem.at[2])
    down_load = pltpu.make_async_copy(down_hbm.at[0], down_v, load_sem.at[3])

    pl.semaphore_wait(barrier, N_NODE - 1 + N_EXPERT - 1)

    after = ((node + 1) % N_NODE, column)
    before = ((node + N_NODE - 1) % N_NODE, column)

    def halo(c, which, side):
        return pltpu.make_async_remote_copy(
            src_ref=kv.at[0, c, which], dst_ref=kv.at[1 + side, c, which],
            send_sem=halo_send.at[side, c, which], recv_sem=halo_recv.at[side, c, which],
            device_id=after if side == 0 else before, device_id_type=MESH,
        )

    def start_halo(c, carry):
        for which in range(2):
            kv_load(c, which).wait()
            halo(c, which, 0).start()
            halo(c, which, 1).start()
        return carry

    lax.fori_loop(0, CHUNKS, start_halo, 0)
    for load in small_loads:
        load.start()
    lax.fori_loop(0, CHUNKS, start_q, 0)
    tok_load.start()
    wo_load.start()
    up_load.start()
    down_load.start()

    for step in range(1, N_EXPERT):
        pl.semaphore_signal(row_sem, inc=1, device_id=(node, (column + step) % N_EXPERT), device_id_type=MESH)

    for load in small_loads:
        load.wait()

    owner = expert_v[...]
    dc = (owner % 2 - core + 2) % 2
    dy = (owner // 2 % 4 - y + 4) % 4
    dx = (owner // 8 % 4 - x + 4) % 4
    dz = (owner // 32 - z + 4) % 4
    part_of = (dy + 8 - dz - dx) % 4
    cell = ((part_of * PART_DEVICES + dx * 8 + dz * 2 + dc) * CAP + slot_v[...]).astype(jnp.float32)
    for t in range(TILES):
        col_v[pl.ds(t * TILE, TILE), :] = jnp.broadcast_to(cell[t : t + 1, :], (TILE, LANES)).T

    lane = lax.broadcasted_iota(jnp.int32, (TILE, LANES), 1)
    left = lane < HEAD_DIM
    left_mask = jnp.where(left, 1.0, 0.0).astype(jnp.bfloat16)
    right_mask = jnp.where(left, 0.0, 1.0).astype(jnp.bfloat16)

    tok_load.wait()
    hidden_v[...] = tok_v[...].astype(jnp.float32)
    wo_load.wait()

    def lanes_of(c):
        return pl.ds(pl.multiple_of(c * LANES, LANES), LANES)

    def listed(t, j):
        tile = nbr_ref[t, j]
        step = (tile // (TILES * N_EXPERT) - node + N_NODE) % N_NODE
        block = jnp.where(step == 0, 0, jnp.where(step == 1, 2, 1))
        bit = live_ref[t, j]
        return jnp.where(bit > 0, block * TILES + tile % TILES, nbr_ref[t, 0] % TILES), bit

    def attend(c, carry):
        @pl.when(c > 0)
        def _():
            for t in range(TILES):
                rows = pl.ds(t * TILE, TILE)
                hidden_v[rows, :] += jnp.dot(
                    attn_v[rows, lanes_of(c - 1)], wo_v[lanes_of(c - 1), :], preferred_element_type=jnp.float32
                )

        q_load(c).wait()
        halo(c, 0, 0).wait_recv()
        halo(c, 0, 1).wait_recv()
        for b in range(3):
            near_k[pl.ds(b * TILES, TILES)] = kv[b, c, 0].reshape(TILES, TILE, LANES)
        for t in range(TILES):
            near_keys = jnp.concatenate([near_k[listed(t, j)[0]] for j in range(NB)], axis=0)
            query = q_v[c, pl.ds(t * TILE, TILE), :]
            both = jnp.concatenate([query * left_mask, query * right_mask], axis=0)
            scores = lax.dot_general(both, near_keys, (((1,), (1,)), ((), ())), preferred_element_type=jnp.float32)
            peak = jnp.max(scores, axis=1, keepdims=True)
            weights_v[t] = jnp.exp2((scores - peak) * SCALE).astype(jnp.bfloat16)
        halo(c, 1, 0).wait_recv()
        halo(c, 1, 1).wait_recv()
        for b in range(3):
            near_v[pl.ds(b * TILES, TILES)] = kv[b, c, 1].reshape(TILES, TILE, LANES)
        for t in range(TILES):
            value_tiles = []
            for j in range(NB):
                position, bit = listed(t, j)
                shown = jnp.full((TILE, LANES), jnp.where(bit > 0, 1.0, 0.0), jnp.float32).astype(jnp.bfloat16)
                value_tiles.append(jnp.concatenate([near_v[position] * shown, shown], axis=1))
            mixed = jnp.dot(weights_v[t], jnp.concatenate(value_tiles, axis=0), preferred_element_type=jnp.float32)
            ratio = mixed[:, :LANES] / mixed[:, LANES:]
            attn_v[pl.ds(t * TILE, TILE), lanes_of(c)] = jnp.where(left, ratio[:TILE], ratio[TILE:]).astype(jnp.bfloat16)
        return carry

    lax.fori_loop(0, CHUNKS, attend, 0)

    last = pl.ds((CHUNKS - 1) * LANES, LANES)
    for t in range(TILES):
        rows = pl.ds(t * TILE, TILE)
        hidden = hidden_v[rows, :] + jnp.dot(attn_v[rows, last], wo_v[last, :], preferred_element_type=jnp.float32)
        hidden_v[rows, :] = hidden
        spread = jnp.mean(hidden * hidden, axis=1, keepdims=True)
        normed_v[rows, :] = (hidden * lax.rsqrt(spread + 1e-06) * gain_v[...]).astype(jnp.bfloat16)

    pl.semaphore_wait(row_sem, N_EXPERT - 1)
    up_z = [(z + d) % 4 * 4 for d in range(4)]
    up_x = [(x + d) % 4 for d in range(4)]
    up_core = [(core + d) % 2 for d in range(2)]
    down_z = [(z + 4 - d) % 4 * 4 for d in range(4)]
    down_x = [(x + 4 - d) % 4 for d in range(4)]

    def dispatch(part, i, up_y):
        oz, ox, oy, oc = offset_of(part, i)
        at = part * PART_DEVICES + i
        return pltpu.make_async_remote_copy(
            src_ref=send_v.at[at], dst_ref=recv_v.at[at], send_sem=disp_send.at[part], recv_sem=disp_recv.at[part],
            device_id=(up_z[oz] + up_x[ox], up_y[oy % 4] + up_core[oc]), device_id_type=MESH,
        )

    cell_row = jnp.concatenate([cell[t : t + 1, :] for t in range(TILES)], axis=1)
    for part in range(PARTS):
        wanted = lax.broadcasted_iota(jnp.int32, (PART_ROWS, TOK), 0).astype(jnp.float32) + part * PART_ROWS
        one_hot = jnp.where(wanted == cell_row, 1.0, 0.0).astype(jnp.bfloat16)
        rows = jnp.dot(one_hot, normed_v[...], preferred_element_type=jnp.float32).astype(jnp.bfloat16)
        send_v[pl.ds(part * PART_DEVICES, PART_DEVICES)] = rows.reshape(PART_DEVICES, CAP, D)
        up_y = [(y + part + d) % 4 * 2 for d in range(4)]
        for i in range(PART_DEVICES):
            if part == 0 and i == 0:
                pltpu.make_async_copy(send_v.at[0], recv_v.at[0], disp_recv.at[0]).start()
            else:
                dispatch(part, i, up_y).start()

    for t in range(TILES):
        rows = pl.ds(t * TILE, TILE)
        logits = jnp.dot(normed_v[rows, :], router_v[...], preferred_element_type=jnp.float32)
        chosen_row = jnp.broadcast_to(owner[t : t + 1, :].astype(jnp.float32), (TILE, LANES))
        chosen = jnp.where(lane.astype(jnp.float32) == chosen_row.T, logits, 0.0)
        gate_v[rows, :] = jnp.broadcast_to(jax.nn.sigmoid(jnp.sum(chosen, axis=1, keepdims=True)), (TILE, LANES))

    up_load.wait()
    down_load.wait()

    def part_slots(part):
        return pl.ds(part * PART_DEVICES, PART_DEVICES)

    def serve(part, carry):
        here = part_slots(part)
        pltpu.make_async_copy(recv_v.at[here], recv_v.at[here], disp_recv.at[part]).wait()

        def lift(f, carry):
            columns = pl.ds(pl.multiple_of(f * FF_BLOCK, FF_BLOCK), FF_BLOCK)
            rows = recv_v[here].reshape(PART_ROWS, D)
            lifted_v[:, columns] = gelu(
                jnp.dot(rows, up_v[:, columns], preferred_element_type=jnp.float32)
            ).astype(jnp.bfloat16)
            return carry

        lax.fori_loop(0, FF // FF_BLOCK, lift, 0)

        def lower(n, carry):
            columns = pl.ds(pl.multiple_of(n * OUT_BLOCK, OUT_BLOCK), OUT_BLOCK)
            lowered = jnp.dot(lifted_v[...], down_v[:, columns], preferred_element_type=jnp.float32)
            res_v[here, :, columns] = lowered.astype(jnp.bfloat16).reshape(PART_DEVICES, CAP, OUT_BLOCK)
            return carry

        lax.fori_loop(0, D // OUT_BLOCK, lower, 0)

        down_y = [(y + 8 - part - d) % 4 * 2 for d in range(4)]
        for i in range(PART_DEVICES):
            oz, ox, oy, oc = offset_of(part, i)
            at = part * PART_DEVICES + i
            back = pltpu.make_async_remote_copy(
                src_ref=res_v.at[at], dst_ref=ret_v.at[at], send_sem=ret_send.at[part], recv_sem=ret_recv.at[part],
                device_id=(down_z[oz] + down_x[ox], down_y[oy % 4] + up_core[oc]), device_id_type=MESH,
            )
            if i > 0:
                back.start()
            else:
                pl.when(part > 0)(back.start)
                own = pltpu.make_async_copy(res_v.at[0], ret_v.at[0], ret_recv.at[0])
                pl.when(part == 0)(own.start)
        return carry

    lax.fori_loop(0, PARTS, serve, 0)

    for part in range(PARTS):
        here = part_slots(part)
        pltpu.make_async_copy(ret_v.at[here], ret_v.at[here], ret_recv.at[part]).wait()
        for t in range(TILES):
            rows = pl.ds(t * TILE, TILE)
            place = col_v[rows, :]
            one_hot = jnp.concatenate(
                [
                    jnp.where(place == lane.astype(jnp.float32) + (part * PART_ROWS + s * LANES), 1.0, 0.0).astype(jnp.bfloat16)
                    for s in range(PART_ROWS // LANES)
                ],
                axis=1,
            )
            taken = jnp.dot(one_hot, ret_v[here].reshape(PART_ROWS, D), preferred_element_type=jnp.float32)
            if part == 0:
                acc_v[rows, :] = taken
            elif part < PARTS - 1:
                acc_v[rows, :] += taken
            else:
                gate = gate_v[rows, :1]
                out_ref[rows, :] = (hidden_v[rows, :] + gate * (acc_v[rows, :] + taken)).astype(jnp.bfloat16)

    def end_halo(c, carry):
        for which in range(2):
            halo(c, which, 0).wait_send()
            halo(c, which, 1).wait_send()
        return carry

    lax.fori_loop(0, CHUNKS, end_halo, 0)
    for part in range(PARTS):
        sent = pl.ds(part * PART_DEVICES + (1 if part == 0 else 0), PART_DEVICES - (1 if part == 0 else 0))
        pltpu.make_async_copy(send_v.at[sent], send_v.at[sent], disp_send.at[part]).wait()
        pltpu.make_async_copy(res_v.at[sent], res_v.at[sent], ret_send.at[part]).wait()


def shards(tokens, queries, keys, values, neighbours, live_bits, out_proj, norm_gain, router, expert, slot, w_up, w_down):
    hbm = pl.BlockSpec(memory_space=pltpu.HBM)
    bf16, f32 = jnp.bfloat16, jnp.float32
    dma = pltpu.SemaphoreType.DMA
    return pl.pallas_call(
        kernel,
        name="layer",
        out_shape=jax.ShapeDtypeStruct((TOK, D), bf16),
        in_specs=[hbm] * 13,
        out_specs=pl.BlockSpec(memory_space=pltpu.VMEM),
        scratch_shapes=[
            pltpu.SMEM((TILES, NB), jnp.int32),
            pltpu.SMEM((TILES, NB), jnp.int32),
            pltpu.VMEM((1, D), f32),
            pltpu.VMEM((D, LANES), bf16),
            pltpu.VMEM((TILES, TILE), jnp.int32),
            pltpu.VMEM((TILES, TILE), jnp.int32),
            pltpu.VMEM((3, CHUNKS, 2, TOK, LANES), bf16),
            pltpu.VMEM((CHUNKS, TOK, LANES), bf16),
            pltpu.VMEM((TOK, D), bf16),
            pltpu.VMEM((D, D), bf16),
            pltpu.VMEM((TOK, D), bf16),
            pltpu.VMEM((3 * TILES, TILE, LANES), bf16),
            pltpu.VMEM((3 * TILES, TILE, LANES), bf16),
            pltpu.VMEM((TILES, 2 * TILE, NB * TILE), bf16),
            pltpu.VMEM((TOK, D), f32),
            pltpu.VMEM((TOK, D), bf16),
            pltpu.VMEM((TOK, LANES), f32),
            pltpu.VMEM((TOK, LANES), f32),
            pltpu.VMEM((DEVICES, CAP, D), bf16),
            pltpu.VMEM((DEVICES, CAP, D), bf16),
            pltpu.VMEM((DEVICES, CAP, D), bf16),
            pltpu.VMEM((DEVICES, CAP, D), bf16),
            pltpu.VMEM((D, FF), bf16),
            pltpu.VMEM((FF, D), bf16),
            pltpu.VMEM((PART_ROWS, FF), bf16),
            pltpu.VMEM((TOK, D), f32),
            dma((10,)),
            dma((CHUNKS, 2)),
            dma((CHUNKS,)),
            dma((2, CHUNKS, 2)),
            dma((2, CHUNKS, 2)),
            dma((PARTS,)),
            dma((PARTS,)),
            dma((PARTS,)),
            dma((PARTS,)),
            pltpu.SemaphoreType.REGULAR,
        ],
        compiler_params=pltpu.CompilerParams(collective_id=0, has_side_effects=True, vmem_limit_bytes=VMEM_LIMIT),
    )(
        neighbours, live_bits, tokens, queries, keys, values, out_proj, norm_gain.reshape(1, D), router,
        expert.reshape(TILES, TILE), slot.reshape(TILES, TILE), w_up, w_down,
    )


def solution(mesh):
    rows = P(("node", "expert"), None)
    flat = P(("node", "expert"))
    deep = P(("node", "expert"), None, None)
    in_specs = (rows, rows, rows, rows, rows, rows, P(), P(), P(), flat, flat, deep, deep)
    return jax.shard_map(shards, mesh=mesh, in_specs=in_specs, out_specs=rows, check_vma=False)
```

```python
import functools

import jax
import jax.numpy as jnp
from jax import lax
from jax.experimental import pallas as pl
from jax.experimental.pallas import tpu as pltpu
from jax.sharding import PartitionSpec as P

MESH = pl.DeviceIdType.MESH
D = 1024
HEADS = 16
HEAD_DIM = 64
FF = 4096
TILE = 128
NB = 8
TOK = 512
TILES = TOK // TILE
CAP = 8
DEVICES = 128
N_NODE = 16
N_EXPERT = 8
LANES = 128
CHUNKS = D // LANES
PARTS = 4
PART_DEVICES = DEVICES // PARTS
PART_ROWS = PART_DEVICES * CAP
FF_BLOCK = 1024
OUT_BLOCK = 512
VMEM_LIMIT = 56_000_000
SCALE = 0.125 * 1.4426950408889634
GELU_A = 0.7978845608028654
GELU_B = 0.044715 * GELU_A


def gelu(v):
    return (0.5 * v) * (1.0 + jnp.tanh(v * (GELU_A + GELU_B * (v * v))))


def offset_of(part, i):
    core = i % 2
    z = (i // 2) % 4
    x = i // 8
    return z, x, z + x, core


def kernel(
    nbr_hbm, live_hbm, tok_hbm, q_hbm, k_hbm, v_hbm, wo_hbm, gain_hbm, router_hbm, expert_hbm, slot_hbm, up_hbm, down_hbm,
    out_ref,
    nbr_ref, live_ref, gain_v, router_v, expert_v, slot_v,
    kv, q_v, tok_v, wo_v, attn_v, near_k, near_v, weights_v, hidden_v, normed_v, gate_v, col_v,
    send_v, recv_v, res_v, ret_v, up_v, down_v, lifted_v, acc_v, sum_v,
    load_sem, kv_sem, q_sem, halo_send, halo_recv, disp_send, disp_recv, ret_send, ret_recv, row_sem, ring_sem,
):
    node = lax.axis_index("node")
    column = lax.axis_index("expert")
    z, x, y, core = node // 4, node % 4, column // 2, column % 2

    def kv_load(c, which):
        source = k_hbm if which == 0 else v_hbm
        return pltpu.make_async_copy(
            source.at[:, pl.ds(pl.multiple_of(c * LANES, LANES), LANES)], kv.at[0, c, which], kv_sem.at[c, which]
        )

    def start_kv(c, carry):
        kv_load(c, 0).start()
        kv_load(c, 1).start()
        return carry

    lax.fori_loop(0, CHUNKS, start_kv, 0)

    barrier = pltpu.get_barrier_semaphore()

    def tell_ring(semaphore, step):
        for peer in (node + step, node + N_NODE - step):
            pl.semaphore_signal(semaphore, inc=1, device_id=(peer % N_NODE, column), device_id_type=MESH)

    tell_ring(barrier, 1)
    for step in range(1, N_EXPERT):
        pl.semaphore_signal(barrier, inc=1, device_id=(node, (column + step) % N_EXPERT), device_id_type=MESH)

    def q_load(c):
        return pltpu.make_async_copy(
            q_hbm.at[:, pl.ds(pl.multiple_of(c * LANES, LANES), LANES)], q_v.at[c], q_sem.at[c]
        )

    def start_q(c, carry):
        q_load(c).start()
        return carry

    small_loads = [
        pltpu.make_async_copy(source, target, load_sem.at[4 + i])
        for i, (source, target) in enumerate(
            (
                (nbr_hbm, nbr_ref), (live_hbm, live_ref), (gain_hbm, gain_v), (router_hbm, router_v),
                (expert_hbm, expert_v), (slot_hbm, slot_v),
            )
        )
    ]
    tok_load = pltpu.make_async_copy(tok_hbm, tok_v, load_sem.at[0])
    wo_load = pltpu.make_async_copy(wo_hbm, wo_v, load_sem.at[1])
    up_load = pltpu.make_async_copy(up_hbm.at[0], up_v, load_sem.at[2])
    down_load = pltpu.make_async_copy(down_hbm.at[0], down_v, load_sem.at[3])

    pl.semaphore_wait(barrier, 2 + N_EXPERT - 1)

    after = ((node + 1) % N_NODE, column)
    before = ((node + N_NODE - 1) % N_NODE, column)

    def halo(c, which, side):
        return pltpu.make_async_remote_copy(
            src_ref=kv.at[0, c, which], dst_ref=kv.at[1 + side, c, which],
            send_sem=halo_send.at[side, c, which], recv_sem=halo_recv.at[side, c, which],
            device_id=after if side == 0 else before, device_id_type=MESH,
        )

    def start_halo(c, carry):
        for which in range(2):
            kv_load(c, which).wait()
            halo(c, which, 0).start()
            halo(c, which, 1).start()
        return carry

    lax.fori_loop(0, CHUNKS, start_halo, 0)
    for load in small_loads:
        load.start()
    lax.fori_loop(0, CHUNKS, start_q, 0)
    tok_load.start()
    wo_load.start()
    up_load.start()
    down_load.start()

    tell_ring(ring_sem.at[0], 1)

    def spread_word(level):
        pl.semaphore_wait(ring_sem.at[level], 2)
        if level < 2:
            tell_ring(ring_sem.at[level + 1], 2 << level)
        else:
            for step in range(1, N_EXPERT):
                pl.semaphore_signal(row_sem, inc=1, device_id=(node, (column + step) % N_EXPERT), device_id_type=MESH)

    for load in small_loads:
        load.wait()

    owner = expert_v[...]
    dc = (owner % 2 - core + 2) % 2
    dy = (owner // 2 % 4 - y + 4) % 4
    dx = (owner // 8 % 4 - x + 4) % 4
    dz = (owner // 32 - z + 4) % 4
    part_of = (dy + 8 - dz - dx) % 4
    cell = ((part_of * PART_DEVICES + dx * 8 + dz * 2 + dc) * CAP + slot_v[...]).astype(jnp.float32)
    for t in range(TILES):
        col_v[pl.ds(t * TILE, TILE), :] = jnp.broadcast_to(cell[t : t + 1, :], (TILE, LANES)).T

    lane = lax.broadcasted_iota(jnp.int32, (TILE, LANES), 1)
    left = lane < HEAD_DIM
    left_mask = jnp.where(left, 1.0, 0.0).astype(jnp.bfloat16)
    right_mask = jnp.where(left, 0.0, 1.0).astype(jnp.bfloat16)

    tok_load.wait()
    hidden_v[...] = tok_v[...].astype(jnp.float32)
    wo_load.wait()

    def lanes_of(c):
        return pl.ds(pl.multiple_of(c * LANES, LANES), LANES)

    def listed(t, j):
        tile = nbr_ref[t, j]
        step = (tile // (TILES * N_EXPERT) - node + N_NODE) % N_NODE
        block = jnp.where(step == 0, 0, jnp.where(step == 1, 2, 1))
        bit = live_ref[t, j]
        return jnp.where(bit > 0, block * TILES + tile % TILES, nbr_ref[t, 0] % TILES), bit

    def attend(c, carry):
        @pl.when(c > 0)
        def _():
            for t in range(TILES):
                rows = pl.ds(t * TILE, TILE)
                hidden_v[rows, :] += jnp.dot(
                    attn_v[rows, lanes_of(c - 1)], wo_v[lanes_of(c - 1), :], preferred_element_type=jnp.float32
                )

        q_load(c).wait()
        halo(c, 0, 0).wait_recv()
        halo(c, 0, 1).wait_recv()
        for b in range(3):
            near_k[pl.ds(b * TILES, TILES)] = kv[b, c, 0].reshape(TILES, TILE, LANES)
        for t in range(TILES):
            near_keys = jnp.concatenate([near_k[listed(t, j)[0]] for j in range(NB)], axis=0)
            query = q_v[c, pl.ds(t * TILE, TILE), :]
            both = jnp.concatenate([query * left_mask, query * right_mask], axis=0)
            scores = lax.dot_general(both, near_keys, (((1,), (1,)), ((), ())), preferred_element_type=jnp.float32)
            peak = jnp.max(scores, axis=1, keepdims=True)
            weights_v[t] = jnp.exp2((scores - peak) * SCALE).astype(jnp.bfloat16)
        halo(c, 1, 0).wait_recv()
        halo(c, 1, 1).wait_recv()
        for b in range(3):
            near_v[pl.ds(b * TILES, TILES)] = kv[b, c, 1].reshape(TILES, TILE, LANES)
        for t in range(TILES):
            value_tiles = []
            for j in range(NB):
                position, bit = listed(t, j)
                shown = jnp.full((TILE, LANES), jnp.where(bit > 0, 1.0, 0.0), jnp.float32).astype(jnp.bfloat16)
                value_tiles.append(jnp.concatenate([near_v[position] * shown, shown], axis=1))
            mixed = jnp.dot(weights_v[t], jnp.concatenate(value_tiles, axis=0), preferred_element_type=jnp.float32)
            ratio = mixed[:, :LANES] / mixed[:, LANES:]
            attn_v[pl.ds(t * TILE, TILE), lanes_of(c)] = jnp.where(left, ratio[:TILE], ratio[TILE:]).astype(jnp.bfloat16)
        for level in range(3):
            pl.when(c == level)(functools.partial(spread_word, level))
        return carry

    lax.fori_loop(0, CHUNKS, attend, 0)

    last = pl.ds((CHUNKS - 1) * LANES, LANES)
    for t in range(TILES):
        rows = pl.ds(t * TILE, TILE)
        hidden = hidden_v[rows, :] + jnp.dot(attn_v[rows, last], wo_v[last, :], preferred_element_type=jnp.float32)
        hidden_v[rows, :] = hidden
        spread = jnp.mean(hidden * hidden, axis=1, keepdims=True)
        normed_v[rows, :] = (hidden * lax.rsqrt(spread + 1e-06) * gain_v[...]).astype(jnp.bfloat16)

    pl.semaphore_wait(row_sem, N_EXPERT - 1)
    up_z = [(z + d) % 4 * 4 for d in range(4)]
    up_x = [(x + d) % 4 for d in range(4)]
    up_core = [(core + d) % 2 for d in range(2)]
    down_z = [(z + 4 - d) % 4 * 4 for d in range(4)]
    down_x = [(x + 4 - d) % 4 for d in range(4)]

    def dispatch(part, i, up_y):
        oz, ox, oy, oc = offset_of(part, i)
        at = part * PART_DEVICES + i
        return pltpu.make_async_remote_copy(
            src_ref=send_v.at[at], dst_ref=recv_v.at[at], send_sem=disp_send.at[part], recv_sem=disp_recv.at[part],
            device_id=(up_z[oz] + up_x[ox], up_y[oy % 4] + up_core[oc]), device_id_type=MESH,
        )

    cell_row = jnp.concatenate([cell[t : t + 1, :] for t in range(TILES)], axis=1)
    for part in range(PARTS):
        wanted = lax.broadcasted_iota(jnp.int32, (PART_ROWS, TOK), 0).astype(jnp.float32) + part * PART_ROWS
        one_hot = jnp.where(wanted == cell_row, 1.0, 0.0).astype(jnp.bfloat16)
        rows = jnp.dot(one_hot, normed_v[...], preferred_element_type=jnp.float32).astype(jnp.bfloat16)
        send_v[pl.ds(part * PART_DEVICES, PART_DEVICES)] = rows.reshape(PART_DEVICES, CAP, D)
        up_y = [(y + part + d) % 4 * 2 for d in range(4)]
        for i in range(PART_DEVICES):
            if part == 0 and i == 0:
                pltpu.make_async_copy(send_v.at[0], recv_v.at[0], disp_recv.at[0]).start()
            else:
                dispatch(part, i, up_y).start()

    for t in range(TILES):
        rows = pl.ds(t * TILE, TILE)
        logits = jnp.dot(normed_v[rows, :], router_v[...], preferred_element_type=jnp.float32)
        chosen_row = jnp.broadcast_to(owner[t : t + 1, :].astype(jnp.float32), (TILE, LANES))
        chosen = jnp.where(lane.astype(jnp.float32) == chosen_row.T, logits, 0.0)
        gate_v[rows, :] = jnp.broadcast_to(jax.nn.sigmoid(jnp.sum(chosen, axis=1, keepdims=True)), (TILE, LANES))

    up_load.wait()
    down_load.wait()

    def part_slots(part):
        return pl.ds(part * PART_DEVICES, PART_DEVICES)

    def serve(part, carry):
        here = part_slots(part)
        pltpu.make_async_copy(recv_v.at[here], recv_v.at[here], disp_recv.at[part]).wait()

        rows = recv_v[here].reshape(PART_ROWS, D)
        blocks = FF // FF_BLOCK

        def lift(f):
            columns = slice(f * FF_BLOCK, (f + 1) * FF_BLOCK)
            lifted_v[:, columns] = gelu(
                jnp.dot(rows, up_v[:, columns], preferred_element_type=jnp.float32)
            ).astype(jnp.bfloat16)

        lift(0)
        for f in range(1, blocks + 1):
            inner = slice((f - 1) * FF_BLOCK, f * FF_BLOCK)
            lowered = jnp.dot(lifted_v[:, inner], down_v[inner, :], preferred_element_type=jnp.float32)
            if f == 1:
                sum_v[...] = lowered
            elif f < blocks:
                sum_v[...] += lowered
            else:
                res_v[here] = (sum_v[...] + lowered).astype(jnp.bfloat16).reshape(PART_DEVICES, CAP, D)
            if f < blocks:
                lift(f)

        down_y = [(y + 8 - part - d) % 4 * 2 for d in range(4)]
        for i in range(PART_DEVICES):
            oz, ox, oy, oc = offset_of(part, i)
            at = part * PART_DEVICES + i
            back = pltpu.make_async_remote_copy(
                src_ref=res_v.at[at], dst_ref=ret_v.at[at], send_sem=ret_send.at[part], recv_sem=ret_recv.at[part],
                device_id=(down_z[oz] + down_x[ox], down_y[oy % 4] + up_core[oc]), device_id_type=MESH,
            )
            if i > 0:
                back.start()
            else:
                pl.when(part > 0)(back.start)
                own = pltpu.make_async_copy(res_v.at[0], ret_v.at[0], ret_recv.at[0])
                pl.when(part == 0)(own.start)
        return carry

    lax.fori_loop(0, PARTS, serve, 0)

    for part in range(PARTS):
        here = part_slots(part)
        pltpu.make_async_copy(ret_v.at[here], ret_v.at[here], ret_recv.at[part]).wait()
        for t in range(TILES):
            rows = pl.ds(t * TILE, TILE)
            place = col_v[rows, :]
            one_hot = jnp.concatenate(
                [
                    jnp.where(place == lane.astype(jnp.float32) + (part * PART_ROWS + s * LANES), 1.0, 0.0).astype(jnp.bfloat16)
                    for s in range(PART_ROWS // LANES)
                ],
                axis=1,
            )
            taken = jnp.dot(one_hot, ret_v[here].reshape(PART_ROWS, D), preferred_element_type=jnp.float32)
            if part == 0:
                acc_v[rows, :] = taken
            elif part < PARTS - 1:
                acc_v[rows, :] += taken
            else:
                gate = gate_v[rows, :1]
                out_ref[rows, :] = (hidden_v[rows, :] + gate * (acc_v[rows, :] + taken)).astype(jnp.bfloat16)

    def end_halo(c, carry):
        for which in range(2):
            halo(c, which, 0).wait_send()
            halo(c, which, 1).wait_send()
        return carry

    lax.fori_loop(0, CHUNKS, end_halo, 0)
    for part in range(PARTS):
        sent = pl.ds(part * PART_DEVICES + (1 if part == 0 else 0), PART_DEVICES - (1 if part == 0 else 0))
        pltpu.make_async_copy(send_v.at[sent], send_v.at[sent], disp_send.at[part]).wait()
        pltpu.make_async_copy(res_v.at[sent], res_v.at[sent], ret_send.at[part]).wait()


def shards(tokens, queries, keys, values, neighbours, live_bits, out_proj, norm_gain, router, expert, slot, w_up, w_down):
    hbm = pl.BlockSpec(memory_space=pltpu.HBM)
    bf16, f32 = jnp.bfloat16, jnp.float32
    dma = pltpu.SemaphoreType.DMA
    return pl.pallas_call(
        kernel,
        name="layer",
        out_shape=pltpu.VMEM((TOK, D), bf16),
        in_specs=[hbm] * 13,
        out_specs=pl.BlockSpec(memory_space=pltpu.VMEM),
        scratch_shapes=[
            pltpu.SMEM((TILES, NB), jnp.int32),
            pltpu.SMEM((TILES, NB), jnp.int32),
            pltpu.VMEM((1, D), f32),
            pltpu.VMEM((D, LANES), bf16),
            pltpu.VMEM((TILES, TILE), jnp.int32),
            pltpu.VMEM((TILES, TILE), jnp.int32),
            pltpu.VMEM((3, CHUNKS, 2, TOK, LANES), bf16),
            pltpu.VMEM((CHUNKS, TOK, LANES), bf16),
            pltpu.VMEM((TOK, D), bf16),
            pltpu.VMEM((D, D), bf16),
            pltpu.VMEM((TOK, D), bf16),
            pltpu.VMEM((3 * TILES, TILE, LANES), bf16),
            pltpu.VMEM((3 * TILES, TILE, LANES), bf16),
            pltpu.VMEM((TILES, 2 * TILE, NB * TILE), bf16),
            pltpu.VMEM((TOK, D), f32),
            pltpu.VMEM((TOK, D), bf16),
            pltpu.VMEM((TOK, LANES), f32),
            pltpu.VMEM((TOK, LANES), f32),
            pltpu.VMEM((DEVICES, CAP, D), bf16),
            pltpu.VMEM((DEVICES, CAP, D), bf16),
            pltpu.VMEM((DEVICES, CAP, D), bf16),
            pltpu.VMEM((DEVICES, CAP, D), bf16),
            pltpu.VMEM((D, FF), bf16),
            pltpu.VMEM((FF, D), bf16),
            pltpu.VMEM((PART_ROWS, FF), bf16),
            pltpu.VMEM((TOK, D), f32),
            pltpu.VMEM((PART_ROWS, D), f32),
            dma((10,)),
            dma((CHUNKS, 2)),
            dma((CHUNKS,)),
            dma((2, CHUNKS, 2)),
            dma((2, CHUNKS, 2)),
            dma((PARTS,)),
            dma((PARTS,)),
            dma((PARTS,)),
            dma((PARTS,)),
            pltpu.SemaphoreType.REGULAR,
            pltpu.SemaphoreType.REGULAR((3,)),
        ],
        compiler_params=pltpu.CompilerParams(collective_id=0, has_side_effects=True, vmem_limit_bytes=VMEM_LIMIT),
    )(
        *[
            pltpu.with_memory_space_constraint(array, pltpu.HBM)
            for array in (
                neighbours, live_bits, tokens, queries, keys, values, out_proj, norm_gain.reshape(1, D), router,
                expert.reshape(TILES, TILE), slot.reshape(TILES, TILE), w_up, w_down,
            )
        ]
    )


def solution(mesh):
    rows = P(("node", "expert"), None)
    flat = P(("node", "expert"))
    deep = P(("node", "expert"), None, None)
    in_specs = (rows, rows, rows, rows, rows, rows, P(), P(), P(), flat, flat, deep, deep)
    return jax.shard_map(shards, mesh=mesh, in_specs=in_specs, out_specs=rows, check_vma=False)
```

```python
import functools

import jax
import jax.numpy as jnp
from jax import lax
from jax.experimental import pallas as pl
from jax.experimental.pallas import tpu as pltpu
from jax.sharding import PartitionSpec as P

MESH = pl.DeviceIdType.MESH
D = 1024
HEADS = 16
HEAD_DIM = 64
FF = 4096
TILE = 128
NB = 8
TOK = 512
TILES = TOK // TILE
CAP = 8
DEVICES = 128
N_NODE = 16
N_EXPERT = 8
LANES = 128
CHUNKS = D // LANES
PARTS = 4
PART_DEVICES = DEVICES // PARTS
PART_ROWS = PART_DEVICES * CAP
FF_BLOCK = 1024
OUT_BLOCK = 512
VMEM_LIMIT = 56_000_000
SCALE = 0.125 * 1.4426950408889634
GELU_A = 0.7978845608028654
GELU_B = 0.044715 * GELU_A


def gelu(v):
    return (0.5 * v) * (1.0 + jnp.tanh(v * (GELU_A + GELU_B * (v * v))))


def offset_of(part, i):
    core = i // 16
    z = i % 4
    x = i // 4 % 4
    y = z + x
    return z, x, y, core


def kernel(
    nbr_hbm, live_hbm, tok_hbm, q_hbm, k_hbm, v_hbm, wo_hbm, gain_hbm, router_hbm, expert_hbm, slot_hbm, up_hbm, down_hbm,
    out_ref,
    nbr_ref, live_ref, gain_v, router_v, expert_v, slot_v,
    kv, q_v, tok_v, wo_v, attn_v, near_k, near_v, weights_v, hidden_v, normed_v, gate_v, col_v,
    send_v, recv_v, res_v, ret_v, up_v, down_v, lifted_v, acc_v, sum_v,
    load_sem, kv_sem, q_sem, halo_send, halo_recv, disp_send, disp_recv, ret_send, ret_recv, row_sem, ring_sem,
):
    node = lax.axis_index("node")
    column = lax.axis_index("expert")
    z, x, y, core = node // 4, node % 4, column // 2, column % 2

    def kv_load(c, which):
        source = k_hbm if which == 0 else v_hbm
        return pltpu.make_async_copy(
            source.at[:, pl.ds(pl.multiple_of(c * LANES, LANES), LANES)], kv.at[0, c, which], kv_sem.at[c, which]
        )

    def start_kv(c, carry):
        kv_load(c, 0).start()
        kv_load(c, 1).start()
        return carry

    lax.fori_loop(0, CHUNKS, start_kv, 0)

    barrier = pltpu.get_barrier_semaphore()

    def tell_ring(semaphore, step):
        for peer in (node + step, node + N_NODE - step):
            pl.semaphore_signal(semaphore, inc=1, device_id=(peer % N_NODE, column), device_id_type=MESH)

    tell_ring(barrier, 1)
    for step in range(1, N_EXPERT):
        pl.semaphore_signal(barrier, inc=1, device_id=(node, (column + step) % N_EXPERT), device_id_type=MESH)

    def q_load(c):
        return pltpu.make_async_copy(
            q_hbm.at[:, pl.ds(pl.multiple_of(c * LANES, LANES), LANES)], q_v.at[c], q_sem.at[c]
        )

    def start_q(c, carry):
        q_load(c).start()
        return carry

    small_loads = [
        pltpu.make_async_copy(source, target, load_sem.at[4 + i])
        for i, (source, target) in enumerate(
            (
                (nbr_hbm, nbr_ref), (live_hbm, live_ref), (gain_hbm, gain_v), (router_hbm, router_v),
                (expert_hbm, expert_v), (slot_hbm, slot_v),
            )
        )
    ]
    tok_load = pltpu.make_async_copy(tok_hbm, tok_v, load_sem.at[0])
    wo_load = pltpu.make_async_copy(wo_hbm, wo_v, load_sem.at[1])
    up_load = pltpu.make_async_copy(up_hbm.at[0], up_v, load_sem.at[2])
    down_load = pltpu.make_async_copy(down_hbm.at[0], down_v, load_sem.at[3])

    pl.semaphore_wait(barrier, 2 + N_EXPERT - 1)

    after = ((node + 1) % N_NODE, column)
    before = ((node + N_NODE - 1) % N_NODE, column)

    def halo(c, which, side):
        return pltpu.make_async_remote_copy(
            src_ref=kv.at[0, c, which], dst_ref=kv.at[1 + side, c, which],
            send_sem=halo_send.at[side, c, which], recv_sem=halo_recv.at[side, c, which],
            device_id=after if side == 0 else before, device_id_type=MESH,
        )

    def start_halo(c, carry):
        for which in range(2):
            kv_load(c, which).wait()
            halo(c, which, 0).start()
            halo(c, which, 1).start()
        return carry

    lax.fori_loop(0, CHUNKS, start_halo, 0)
    for load in small_loads:
        load.start()
    lax.fori_loop(0, CHUNKS, start_q, 0)
    tok_load.start()
    wo_load.start()
    up_load.start()
    down_load.start()

    tell_ring(ring_sem.at[0], 1)

    def spread_word(level):
        pl.semaphore_wait(ring_sem.at[level], 2)
        if level < 2:
            tell_ring(ring_sem.at[level + 1], 2 << level)
        else:
            for step in range(1, N_EXPERT):
                pl.semaphore_signal(row_sem, inc=1, device_id=(node, (column + step) % N_EXPERT), device_id_type=MESH)

    for load in small_loads:
        load.wait()

    owner = expert_v[...]
    dc = (owner % 2 - core + 2) % 2
    dy = (owner // 2 % 4 - y + 4) % 4
    dx = (owner // 8 % 4 - x + 4) % 4
    dz = (owner // 32 - z + 4) % 4
    part_of = (dy + 8 - dz - dx) % 4
    cell = ((part_of * PART_DEVICES + dc * 16 + dx * 4 + dz) * CAP + slot_v[...]).astype(jnp.float32)
    for t in range(TILES):
        col_v[pl.ds(t * TILE, TILE), :] = jnp.broadcast_to(cell[t : t + 1, :], (TILE, LANES)).T

    lane = lax.broadcasted_iota(jnp.int32, (TILE, LANES), 1)
    left = lane < HEAD_DIM
    left_mask = jnp.where(left, 1.0, 0.0).astype(jnp.bfloat16)
    right_mask = jnp.where(left, 0.0, 1.0).astype(jnp.bfloat16)

    tok_load.wait()
    hidden_v[...] = tok_v[...].astype(jnp.float32)
    wo_load.wait()

    def lanes_of(c):
        return pl.ds(pl.multiple_of(c * LANES, LANES), LANES)

    def listed(t, j):
        tile = nbr_ref[t, j]
        step = (tile // (TILES * N_EXPERT) - node + N_NODE) % N_NODE
        block = jnp.where(step == 0, 0, jnp.where(step == 1, 2, 1))
        bit = live_ref[t, j]
        return jnp.where(bit > 0, block * TILES + tile % TILES, nbr_ref[t, 0] % TILES), bit

    def attend(c, carry):
        @pl.when(c > 0)
        def _():
            for t in range(TILES):
                rows = pl.ds(t * TILE, TILE)
                hidden_v[rows, :] += jnp.dot(
                    attn_v[rows, lanes_of(c - 1)], wo_v[lanes_of(c - 1), :], preferred_element_type=jnp.float32
                )

        q_load(c).wait()
        halo(c, 0, 0).wait_recv()
        halo(c, 0, 1).wait_recv()
        for b in range(3):
            near_k[pl.ds(b * TILES, TILES)] = kv[b, c, 0].reshape(TILES, TILE, LANES)
        for t in range(TILES):
            near_keys = jnp.concatenate([near_k[listed(t, j)[0]] for j in range(NB)], axis=0)
            query = q_v[c, pl.ds(t * TILE, TILE), :]
            both = jnp.concatenate([query * left_mask, query * right_mask], axis=0)
            scores = lax.dot_general(both, near_keys, (((1,), (1,)), ((), ())), preferred_element_type=jnp.float32)
            peak = jnp.max(scores, axis=1, keepdims=True)
            weights_v[t] = jnp.exp2((scores - peak) * SCALE).astype(jnp.bfloat16)
        halo(c, 1, 0).wait_recv()
        halo(c, 1, 1).wait_recv()
        for b in range(3):
            near_v[pl.ds(b * TILES, TILES)] = kv[b, c, 1].reshape(TILES, TILE, LANES)
        for t in range(TILES):
            value_tiles = []
            for j in range(NB):
                position, bit = listed(t, j)
                shown = jnp.full((TILE, LANES), jnp.where(bit > 0, 1.0, 0.0), jnp.float32).astype(jnp.bfloat16)
                value_tiles.append(jnp.concatenate([near_v[position] * shown, shown], axis=1))
            mixed = jnp.dot(weights_v[t], jnp.concatenate(value_tiles, axis=0), preferred_element_type=jnp.float32)
            ratio = mixed[:, :LANES] / mixed[:, LANES:]
            attn_v[pl.ds(t * TILE, TILE), lanes_of(c)] = jnp.where(left, ratio[:TILE], ratio[TILE:]).astype(jnp.bfloat16)
        for level in range(3):
            pl.when(c == level)(functools.partial(spread_word, level))
        return carry

    lax.fori_loop(0, CHUNKS, attend, 0)

    last = pl.ds((CHUNKS - 1) * LANES, LANES)
    for t in range(TILES):
        rows = pl.ds(t * TILE, TILE)
        hidden = hidden_v[rows, :] + jnp.dot(attn_v[rows, last], wo_v[last, :], preferred_element_type=jnp.float32)
        hidden_v[rows, :] = hidden
        spread = jnp.mean(hidden * hidden, axis=1, keepdims=True)
        normed_v[rows, :] = (hidden * lax.rsqrt(spread + 1e-06) * gain_v[...]).astype(jnp.bfloat16)

    pl.semaphore_wait(row_sem, N_EXPERT - 1)
    up_z = [(z + d) % 4 * 4 for d in range(4)]
    up_x = [(x + d) % 4 for d in range(4)]
    up_y = [(y + d) % 4 * 2 for d in range(4)]
    up_core = [(core + d) % 2 for d in range(2)]
    down_z = [(z + 4 - d) % 4 * 4 for d in range(4)]
    down_x = [(x + 4 - d) % 4 for d in range(4)]

    def dispatch(part, i, up_z, up_x, up_y):
        oz, ox, oy, oc = offset_of(part, i)
        at = part * PART_DEVICES + i
        return pltpu.make_async_remote_copy(
            src_ref=send_v.at[at], dst_ref=recv_v.at[at], send_sem=disp_send.at[part], recv_sem=disp_recv.at[part],
            device_id=(up_z[oz % 4] + up_x[ox % 4], up_y[oy % 4] + up_core[oc]), device_id_type=MESH,
        )

    cell_row = jnp.concatenate([cell[t : t + 1, :] for t in range(TILES)], axis=1)
    for part in range(PARTS):
        wanted = lax.broadcasted_iota(jnp.int32, (PART_ROWS, TOK), 0).astype(jnp.float32) + part * PART_ROWS
        one_hot = jnp.where(wanted == cell_row, 1.0, 0.0).astype(jnp.bfloat16)
        rows = jnp.dot(one_hot, normed_v[...], preferred_element_type=jnp.float32).astype(jnp.bfloat16)
        send_v[pl.ds(part * PART_DEVICES, PART_DEVICES)] = rows.reshape(PART_DEVICES, CAP, D)
        up_y = [(y + part + d) % 4 * 2 for d in range(4)]
        for i in range(PART_DEVICES):
            if part == 0 and i == 0:
                pltpu.make_async_copy(send_v.at[0], recv_v.at[0], disp_recv.at[0]).start()
            else:
                dispatch(part, i, up_z, up_x, up_y).start()

    for t in range(TILES):
        rows = pl.ds(t * TILE, TILE)
        logits = jnp.dot(normed_v[rows, :], router_v[...], preferred_element_type=jnp.float32)
        chosen_row = jnp.broadcast_to(owner[t : t + 1, :].astype(jnp.float32), (TILE, LANES))
        chosen = jnp.where(lane.astype(jnp.float32) == chosen_row.T, logits, 0.0)
        gate_v[rows, :] = jnp.broadcast_to(jax.nn.sigmoid(jnp.sum(chosen, axis=1, keepdims=True)), (TILE, LANES))

    up_load.wait()
    down_load.wait()

    def part_slots(part):
        return pl.ds(part * PART_DEVICES, PART_DEVICES)

    def serve(part, carry):
        here = part_slots(part)
        pltpu.make_async_copy(recv_v.at[here], recv_v.at[here], disp_recv.at[part]).wait()

        rows = recv_v[here].reshape(PART_ROWS, D)
        blocks = FF // FF_BLOCK

        def lift(f):
            columns = slice(f * FF_BLOCK, (f + 1) * FF_BLOCK)
            lifted_v[:, columns] = gelu(
                jnp.dot(rows, up_v[:, columns], preferred_element_type=jnp.float32)
            ).astype(jnp.bfloat16)

        lift(0)
        for f in range(1, blocks + 1):
            inner = slice((f - 1) * FF_BLOCK, f * FF_BLOCK)
            lowered = jnp.dot(lifted_v[:, inner], down_v[inner, :], preferred_element_type=jnp.float32)
            if f == 1:
                sum_v[...] = lowered
            elif f < blocks:
                sum_v[...] += lowered
            else:
                res_v[here] = (sum_v[...] + lowered).astype(jnp.bfloat16).reshape(PART_DEVICES, CAP, D)
            if f < blocks:
                lift(f)

        down_z = [(z + 4 - d) % 4 * 4 for d in range(4)]
        down_x = [(x + 4 - d) % 4 for d in range(4)]
        down_y = [(y + 8 - part - d) % 4 * 2 for d in range(4)]
        for i in range(PART_DEVICES):
            oz, ox, oy, oc = offset_of(part, i)
            at = part * PART_DEVICES + i
            back = pltpu.make_async_remote_copy(
                src_ref=res_v.at[at], dst_ref=ret_v.at[at], send_sem=ret_send.at[part], recv_sem=ret_recv.at[part],
                device_id=(down_z[oz % 4] + down_x[ox % 4], down_y[oy % 4] + up_core[oc]), device_id_type=MESH,
            )
            if i > 0:
                back.start()
            else:
                pl.when(part > 0)(back.start)
                own = pltpu.make_async_copy(res_v.at[0], ret_v.at[0], ret_recv.at[0])
                pl.when(part == 0)(own.start)
        return carry

    lax.fori_loop(0, PARTS, serve, 0)

    for part in range(PARTS):
        here = part_slots(part)
        pltpu.make_async_copy(ret_v.at[here], ret_v.at[here], ret_recv.at[part]).wait()
        for t in range(TILES):
            rows = pl.ds(t * TILE, TILE)
            place = col_v[rows, :]
            one_hot = jnp.concatenate(
                [
                    jnp.where(place == lane.astype(jnp.float32) + (part * PART_ROWS + s * LANES), 1.0, 0.0).astype(jnp.bfloat16)
                    for s in range(PART_ROWS // LANES)
                ],
                axis=1,
            )
            taken = jnp.dot(one_hot, ret_v[here].reshape(PART_ROWS, D), preferred_element_type=jnp.float32)
            if part == 0:
                acc_v[rows, :] = taken
            elif part < PARTS - 1:
                acc_v[rows, :] += taken
            else:
                gate = gate_v[rows, :1]
                out_ref[rows, :] = (hidden_v[rows, :] + gate * (acc_v[rows, :] + taken)).astype(jnp.bfloat16)

    def end_halo(c, carry):
        for which in range(2):
            halo(c, which, 0).wait_send()
            halo(c, which, 1).wait_send()
        return carry

    lax.fori_loop(0, CHUNKS, end_halo, 0)
    for part in range(PARTS):
        sent = pl.ds(part * PART_DEVICES + (1 if part == 0 else 0), PART_DEVICES - (1 if part == 0 else 0))
        pltpu.make_async_copy(send_v.at[sent], send_v.at[sent], disp_send.at[part]).wait()
        pltpu.make_async_copy(res_v.at[sent], res_v.at[sent], ret_send.at[part]).wait()


def shards(tokens, queries, keys, values, neighbours, live_bits, out_proj, norm_gain, router, expert, slot, w_up, w_down):
    hbm = pl.BlockSpec(memory_space=pltpu.HBM)
    bf16, f32 = jnp.bfloat16, jnp.float32
    dma = pltpu.SemaphoreType.DMA
    return pl.pallas_call(
        kernel,
        name="layer",
        out_shape=pltpu.VMEM((TOK, D), bf16),
        in_specs=[hbm] * 13,
        out_specs=pl.BlockSpec(memory_space=pltpu.VMEM),
        scratch_shapes=[
            pltpu.SMEM((TILES, NB), jnp.int32),
            pltpu.SMEM((TILES, NB), jnp.int32),
            pltpu.VMEM((1, D), f32),
            pltpu.VMEM((D, LANES), bf16),
            pltpu.VMEM((TILES, TILE), jnp.int32),
            pltpu.VMEM((TILES, TILE), jnp.int32),
            pltpu.VMEM((3, CHUNKS, 2, TOK, LANES), bf16),
            pltpu.VMEM((CHUNKS, TOK, LANES), bf16),
            pltpu.VMEM((TOK, D), bf16),
            pltpu.VMEM((D, D), bf16),
            pltpu.VMEM((TOK, D), bf16),
            pltpu.VMEM((3 * TILES, TILE, LANES), bf16),
            pltpu.VMEM((3 * TILES, TILE, LANES), bf16),
            pltpu.VMEM((TILES, 2 * TILE, NB * TILE), bf16),
            pltpu.VMEM((TOK, D), f32),
            pltpu.VMEM((TOK, D), bf16),
            pltpu.VMEM((TOK, LANES), f32),
            pltpu.VMEM((TOK, LANES), f32),
            pltpu.VMEM((DEVICES, CAP, D), bf16),
            pltpu.VMEM((DEVICES, CAP, D), bf16),
            pltpu.VMEM((DEVICES, CAP, D), bf16),
            pltpu.VMEM((DEVICES, CAP, D), bf16),
            pltpu.VMEM((D, FF), bf16),
            pltpu.VMEM((FF, D), bf16),
            pltpu.VMEM((PART_ROWS, FF), bf16),
            pltpu.VMEM((TOK, D), f32),
            pltpu.VMEM((PART_ROWS, D), f32),
            dma((10,)),
            dma((CHUNKS, 2)),
            dma((CHUNKS,)),
            dma((2, CHUNKS, 2)),
            dma((2, CHUNKS, 2)),
            dma((PARTS,)),
            dma((PARTS,)),
            dma((PARTS,)),
            dma((PARTS,)),
            pltpu.SemaphoreType.REGULAR,
            pltpu.SemaphoreType.REGULAR((3,)),
        ],
        compiler_params=pltpu.CompilerParams(collective_id=0, has_side_effects=True, vmem_limit_bytes=VMEM_LIMIT),
    )(
        *[
            pltpu.with_memory_space_constraint(array, pltpu.HBM)
            for array in (
                neighbours, live_bits, tokens, queries, keys, values, out_proj, norm_gain.reshape(1, D), router,
                expert.reshape(TILES, TILE), slot.reshape(TILES, TILE), w_up, w_down,
            )
        ]
    )


def solution(mesh):
    rows = P(("node", "expert"), None)
    flat = P(("node", "expert"))
    deep = P(("node", "expert"), None, None)
    in_specs = (rows, rows, rows, rows, rows, rows, P(), P(), P(), flat, flat, deep, deep)
    return jax.shard_map(shards, mesh=mesh, in_specs=in_specs, out_specs=rows, check_vma=False)
```
